16 devices in a mesh: dp: 4 (over z, y), tp: 4 (over x, core).
Axes of the slice: x: 2, y: 2, z: 2, core: 2. Of those that a mesh axis runs over, the one named last changes fastest.
Arguments:
- patches: bfloat16 [96, 256, 768], P('dp', 'tp'), parts along dimension 0
- patch_w: bfloat16 [768, 1024], replicated
- patch_b: bfloat16 [1024], replicated
- pos_emb: bfloat16 [256, 1024], P('tp')
- ln_scale: bfloat16 [2, 1024], replicated
- ln_bias: bfloat16 [2, 1024], replicated
- qkv_w: bfloat16 [3, 1024, 16, 64], P(None, None, 'tp')
- qkv_b: bfloat16 [3, 16, 64], P(None, 'tp')
- out_w: bfloat16 [16, 64, 1024], P('tp')
- out_b: bfloat16 [1024], replicated
- fc1_w: bfloat16 [1024, 4096], P(None, 'tp')
- fc1_b: bfloat16 [4096], P('tp')
- fc2_w: bfloat16 [4096, 1024], P('tp')
- fc2_b: bfloat16 [1024], replicated
- d_out: bfloat16 [96, 256, 1024], P('dp', 'tp'), parts along dimension 0
Outputs:
- output 1: bfloat16 [96, 256, 1024], P('dp', 'tp'), parts along dimension 0
- output 2: bfloat16 [3072, 1024], P('dp'), parts along dimension 0
- output 3: bfloat16 [4096], P('dp'), parts along dimension 0
- output 4: bfloat16 [1024, 1024], P(('dp', 'tp')), parts along dimension 0
- output 5: bfloat16 [8, 1024], P('dp'), parts along dimension 0
- output 6: bfloat16 [8, 1024], P('dp'), parts along dimension 0
- output 7: bfloat16 [12, 1024, 16, 64], P('dp', None, 'tp'), parts along dimension 0
- output 8: bfloat16 [12, 16, 64], P('dp', 'tp'), parts along dimension 0
- output 9: bfloat16 [64, 64, 1024], P(('dp', 'tp')), parts along dimension 0
- output 10: bfloat16 [4096], P('dp'), parts along dimension 0
- output 11: bfloat16 [4096, 4096], P('dp', 'tp'), parts along dimension 0
- output 12: bfloat16 [16384], P(('dp', 'tp')), parts along dimension 0
- output 13: bfloat16 [16384, 1024], P(('dp', 'tp')), parts along dimension 0
- output 14: bfloat16 [4096], P('dp'), parts along dimension 0
There are 4 independent parts. The reference program is written for one: setup_inputs(seed, part) draws one part's arguments, and reference() takes and returns one part's arrays. A program takes and returns all parts, laid end to end along the dimension named above; an argument that names none is the same for every part.
All inputs are finite; a program needn't handle non-finite values.
Results may differ from the reference program's by a relative error of at most 0.02.
Values are sent between devices in bfloat16 or wider.
A program may use at most 1 GiB of HBM per device.

```python
import functools
import jax
import jax.numpy as jnp
from jax import lax

NUM_IMAGES = 24
NUM_TOKENS = 256
PATCH_DIM = 768
MODEL_DIM = 1024
NUM_HEADS = 16
HEAD_DIM = 64
MLP_DIM = 4096
LN_EPS = 1e-6


def draw_normal(key, shape, scale):
    return (jax.random.normal(key, shape, jnp.float32) * scale).astype(jnp.bfloat16)


def setup_inputs(seed: int = 0, part: int = 0) -> dict:
    base_key = jax.random.key(seed)
    part_key = jax.random.fold_in(base_key, part)
    weight_keys = jax.random.split(base_key, 13)
    data_keys = jax.random.split(part_key, 2)
    qk_gain = 1.6 * MODEL_DIM ** -0.5
    qkv_gain = jnp.array([qk_gain, qk_gain, MODEL_DIM ** -0.5], jnp.float32).reshape(3, 1, 1, 1)
    ln_gain = 1.0 + 0.3 * jax.random.normal(weight_keys[3], (2, MODEL_DIM), jnp.float32)
    qkv_raw = jax.random.normal(weight_keys[5], (3, MODEL_DIM, NUM_HEADS, HEAD_DIM), jnp.float32)
    return {
        'patches': draw_normal(data_keys[0], (NUM_IMAGES, NUM_TOKENS, PATCH_DIM), 1.0),
        'patch_w': draw_normal(weight_keys[0], (PATCH_DIM, MODEL_DIM), PATCH_DIM ** -0.5),
        'patch_b': draw_normal(weight_keys[1], (MODEL_DIM,), 0.5),
        'pos_emb': draw_normal(weight_keys[2], (NUM_TOKENS, MODEL_DIM), 0.5),
        'ln_scale': ln_gain.astype(jnp.bfloat16),
        'ln_bias': draw_normal(weight_keys[4], (2, MODEL_DIM), 0.3),
        'qkv_w': (qkv_raw * qkv_gain).astype(jnp.bfloat16),
        'qkv_b': draw_normal(weight_keys[6], (3, NUM_HEADS, HEAD_DIM), 0.3),
        'out_w': draw_normal(weight_keys[7], (NUM_HEADS, HEAD_DIM, MODEL_DIM), MODEL_DIM ** -0.5),
        'out_b': draw_normal(weight_keys[8], (MODEL_DIM,), 0.5),
        'fc1_w': draw_normal(weight_keys[9], (MODEL_DIM, MLP_DIM), MODEL_DIM ** -0.5),
        'fc1_b': draw_normal(weight_keys[10], (MLP_DIM,), 0.5),
        'fc2_w': draw_normal(weight_keys[11], (MLP_DIM, MODEL_DIM), MLP_DIM ** -0.5),
        'fc2_b': draw_normal(weight_keys[12], (MODEL_DIM,), 0.5),
        'd_out': draw_normal(data_keys[1], (NUM_IMAGES, NUM_TOKENS, MODEL_DIM), 1.0),
    }


def layer_norm(x_val, scale, bias):
    row_mean = jnp.mean(x_val, axis=-1, keepdims=True)
    centered = x_val - row_mean
    row_var = jnp.mean(centered * centered, axis=-1, keepdims=True)
    return centered * lax.rsqrt(row_var + LN_EPS) * scale.astype(jnp.float32) + bias.astype(jnp.float32)


def attend_image(qkv_img):
    query = qkv_img[:, 0].astype(jnp.float32)
    keys_img = qkv_img[:, 1].astype(jnp.float32)
    values = qkv_img[:, 2].astype(jnp.float32)
    scores = jnp.einsum('qhc,khc->hqk', query, keys_img) * HEAD_DIM ** -0.5
    probs = jax.nn.softmax(scores, axis=-1).astype(jnp.bfloat16)
    context = jnp.einsum('hqk,khc->qhc', probs.astype(jnp.float32), values)
    return context.astype(jnp.bfloat16)


def forward(patches, params):
    patch_w, patch_b, pos_emb, ln_scale, ln_bias, qkv_w, qkv_b, out_w, out_b, fc1_w, fc1_b, fc2_w, fc2_b = params
    emb = jnp.einsum('btp,pd->btd', patches.astype(jnp.float32), patch_w.astype(jnp.float32))
    emb_f = (emb + patch_b.astype(jnp.float32) + pos_emb.astype(jnp.float32)).astype(jnp.bfloat16).astype(jnp.float32)
    h_one = layer_norm(emb_f, ln_scale[0], ln_bias[0]).astype(jnp.bfloat16)
    qkv = jnp.einsum('btd,sdhc->btshc', h_one.astype(jnp.float32), qkv_w.astype(jnp.float32)) + qkv_b.astype(jnp.float32)
    context = lax.map(jax.checkpoint(attend_image), qkv.astype(jnp.bfloat16))
    attn_out = jnp.einsum('bthc,hcd->btd', context.astype(jnp.float32), out_w.astype(jnp.float32)) + out_b.astype(jnp.float32)
    x_one_f = (emb_f + attn_out).astype(jnp.bfloat16).astype(jnp.float32)
    h_two = layer_norm(x_one_f, ln_scale[1], ln_bias[1]).astype(jnp.bfloat16)
    pre_act = jnp.einsum('btd,df->btf', h_two.astype(jnp.float32), fc1_w.astype(jnp.float32)) + fc1_b.astype(jnp.float32)
    hidden = jax.nn.gelu(pre_act, approximate=True).astype(jnp.bfloat16)
    mlp_out = jnp.einsum('btf,fd->btd', hidden.astype(jnp.float32), fc2_w.astype(jnp.float32)) + fc2_b.astype(jnp.float32)
    return (x_one_f + mlp_out).astype(jnp.bfloat16)


def reference(patches, patch_w, patch_b, pos_emb, ln_scale, ln_bias, qkv_w, qkv_b, out_w, out_b, fc1_w, fc1_b, fc2_w, fc2_b, d_out):
    params = (patch_w, patch_b, pos_emb, ln_scale, ln_bias, qkv_w, qkv_b, out_w, out_b, fc1_w, fc1_b, fc2_w, fc2_b)
    x_two, pull_back = jax.vjp(functools.partial(forward, patches), params)
    grads = pull_back(d_out)[0]
    return (x_two, grads[0], grads[1], grads[2], grads[3], grads[4], grads[5], grads[6], grads[7], grads[8], grads[9], grads[10], grads[11], grads[12])
```

```python
import jax
import jax.numpy as jnp
from jax import lax
from jax.sharding import PartitionSpec as P

LN_EPS = 1e-6
X_PAIRS = [(0, 2), (2, 0), (1, 3), (3, 1)]
CORE_PAIRS = [(0, 1), (1, 0), (2, 3), (3, 2)]
WIDE = jnp.float32
HALF = jnp.bfloat16


def x_swap(val):
    return lax.ppermute(val, 'tp', X_PAIRS)


def core_swap(val):
    return lax.ppermute(val, 'tp', CORE_PAIRS)


def layer_norm(x_val, scale_f, bias_f):
    row_mean = jnp.mean(x_val, axis=-1, keepdims=True)
    centered = x_val - row_mean
    row_var = jnp.mean(centered * centered, axis=-1, keepdims=True)
    return centered * lax.rsqrt(row_var + LN_EPS) * scale_f + bias_f


def gelu_tanh(pre_act):
    return jax.nn.gelu(pre_act, approximate=True)


def dot(spec, lhs, rhs):
    return jnp.einsum(spec, lhs, rhs, preferred_element_type=WIDE)


def partner_weight(weight, axis):
    quarter = weight.shape[axis] // lax.axis_size('dp')
    piece = lax.dynamic_slice_in_dim(weight, lax.axis_index('dp') * quarter, quarter, axis)
    return lax.all_gather(x_swap(piece), 'dp', axis=axis, tiled=True)


def attend(qkv, d_context_of):
    scale = qkv.shape[-1] ** -0.5
    query, keys_all, values = qkv[:, :, 0], qkv[:, :, 1], qkv[:, :, 2]
    scores = dot('bqhc,bkhc->bhqk', query, keys_all) * scale
    probs = jax.nn.softmax(scores, axis=-1)
    probs_h = probs.astype(HALF)
    context = dot('bhqk,bkhc->bqhc', probs_h, values).astype(HALF)

    def backward(d_context):
        d_values = dot('bhqk,bqhc->bkhc', probs_h, d_context).astype(HALF)
        d_probs = dot('bqhc,bkhc->bhqk', d_context, values).astype(HALF).astype(WIDE)
        d_scores = probs * (d_probs - jnp.sum(d_probs * probs, axis=-1, keepdims=True))
        d_scores_h = (d_scores * scale).astype(HALF)
        d_query = dot('bhqk,bkhc->bqhc', d_scores_h, keys_all).astype(HALF)
        d_keys = dot('bhqk,bqhc->bkhc', d_scores_h, query).astype(HALF)
        return jnp.stack([d_query, d_keys, d_values], axis=2)

    return context, backward


def group_step(patches, patch_w, patch_b, pos_emb, ln_scale, ln_bias, qkv_w, qkv_b, out_w, out_b, fc1_w, fc1_b, fc2_w, fc2_b, d_out):
    n_img, n_tok = patches.shape[0], patches.shape[1]
    half_img = n_img // 2
    side = lax.axis_index('tp') // 2
    own_start, other_start = side * half_img, (1 - side) * half_img
    ln_scale_f, ln_bias_f = ln_scale.astype(WIDE), ln_bias.astype(WIDE)

    def own_img(val):
        return lax.dynamic_slice_in_dim(val, own_start, half_img, 0)

    def other_img(val):
        return lax.dynamic_slice_in_dim(val, other_start, half_img, 0)

    pat_recv = x_swap(other_img(patches))
    pos_recv = x_swap(pos_emb)
    qkv_w_p = partner_weight(qkv_w, 1)
    qkv_b_p = x_swap(qkv_b)
    out_w_p = partner_weight(out_w, 1)
    fc1_w_p = partner_weight(fc1_w, 0)
    fc1_b_p = x_swap(fc1_b)
    fc2_w_p = partner_weight(fc2_w, 0)
    d_out_recv = x_swap(d_out)

    def blocks(first, second):
        return jnp.concatenate([first, second], axis=1)

    pat = blocks(own_img(patches), pat_recv)
    pos = jnp.concatenate([pos_emb, pos_recv], axis=0).astype(WIDE)
    emb = dot('btp,pd->btd', pat, patch_w)
    emb_f = (emb + patch_b.astype(WIDE) + pos).astype(HALF).astype(WIDE)
    h_one_f, ln_one_vjp = jax.vjp(layer_norm, emb_f, ln_scale_f[0], ln_bias_f[0])
    h_one_a = h_one_f.astype(HALF)
    h_one_b = core_swap(h_one_a)
    h_one = jnp.concatenate([h_one_a, h_one_b], axis=1)

    qkv_w_all = (qkv_w, qkv_w_p)
    out_w_all = (out_w, out_w_p)
    contexts, backs = [], []
    for w_val, b_val in zip(qkv_w_all, (qkv_b, qkv_b_p)):
        qkv = (dot('btd,sdhc->btshc', h_one, w_val) + b_val.astype(WIDE)).astype(HALF)
        context, back = attend(qkv, None)
        contexts.append(context)
        backs.append(back)

    def out_part(tokens):
        return sum(dot('crid,ide->cre', context[:, tokens], w_val) for context, w_val in zip(contexts, out_w_all))

    first, second = slice(0, 2 * n_tok), slice(2 * n_tok, 4 * n_tok)
    attn_recv = core_swap(out_part(second))
    attn_out = out_part(first) + attn_recv
    x_one_f = (emb_f + (attn_out + out_b.astype(WIDE))).astype(HALF).astype(WIDE)
    h_two_f, ln_two_vjp = jax.vjp(layer_norm, x_one_f, ln_scale_f[1], ln_bias_f[1])
    h_two_a = h_two_f.astype(HALF)
    h_two_b = core_swap(h_two_a)
    h_two_oa = x_swap(h_two_a)
    h_two_ob = core_swap(h_two_oa)

    def mlp_up(h_val, w_val, b_val):
        pre_act = dot('btd,df->btf', h_val, w_val) + b_val.astype(WIDE)
        hidden_f, gelu_vjp = jax.vjp(gelu_tanh, pre_act)
        return hidden_f.astype(HALF), gelu_vjp

    own_a = mlp_up(h_two_a, fc1_w, fc1_b)
    own_b = mlp_up(h_two_b, fc1_w, fc1_b)
    par_a = mlp_up(h_two_a, fc1_w_p, fc1_b_p)
    par_b = mlp_up(h_two_b, fc1_w_p, fc1_b_p)

    def down(own, par):
        return dot('btf,fd->btd', own[0], fc2_w) + dot('btf,fd->btd', par[0], fc2_w_p)

    mlp_recv = core_swap(down(own_b, par_b))
    mlp_out = down(own_a, par_a) + mlp_recv
    x_two = (x_one_f + (mlp_out + fc2_b.astype(WIDE))).astype(HALF)
    x_two_recv = x_swap(x_two[:, n_tok:])
    x_two_own = x_two[:, :n_tok]
    x_two_out = jnp.where(side == 0, jnp.concatenate([x_two_own, x_two_recv], axis=0), jnp.concatenate([x_two_recv, x_two_own], axis=0))

    d_two_a = blocks(own_img(d_out), own_img(d_out_recv))
    d_two_oa = blocks(other_img(d_out_recv), other_img(d_out))
    d_two_b = core_swap(d_two_a)
    d_two_ob = core_swap(d_two_oa)

    def d_up(d_two, gelu_vjp, w_val):
        d_hidden = dot('btd,fd->btf', d_two, w_val).astype(HALF)
        return gelu_vjp(d_hidden.astype(WIDE))[0]

    d_pre_own_a = d_up(d_two_a, own_a[1], fc2_w)
    d_pre_own_b = d_up(d_two_b, own_b[1], fc2_w)
    d_pre_par_a = d_up(d_two_a, par_a[1], fc2_w_p)
    d_pre_par_b = d_up(d_two_b, par_b[1], fc2_w_p)

    def d_down(own, par):
        return dot('btf,df->btd', own.astype(HALF), fc1_w) + dot('btf,df->btd', par.astype(HALF), fc1_w_p)

    d_h_two_recv = core_swap(d_down(d_pre_own_b, d_pre_par_b))
    d_h_two = (d_down(d_pre_own_a, d_pre_par_a) + d_h_two_recv).astype(HALF)
    d_x_ln, d_ln2_scale, d_ln2_bias = ln_two_vjp(d_h_two.astype(WIDE))
    d_x_one = (d_two_a.astype(WIDE) + d_x_ln).astype(HALF)
    d_out_b = jnp.sum(d_x_one, axis=(0, 1), dtype=WIDE)
    d_x_one_b = core_swap(d_x_one)

    d_x_one_all = jnp.concatenate([d_x_one, d_x_one_b], axis=1)
    d_qkv_all, d_out_w_parts = [], []
    for context, back, w_val in zip(contexts, backs, out_w_all):
        d_out_w_parts.append(dot('crid,cre->ide', context, d_x_one_all))
        d_context = dot('cre,ide->crid', d_x_one_all, w_val).astype(HALF)
        d_qkv_all.append(back(d_context))
    d_out_w = d_out_w_parts[0] + x_swap(d_out_w_parts[1])
    d_qkv_b_parts = [jnp.sum(d_qkv, axis=(0, 1), dtype=WIDE) for d_qkv in d_qkv_all]
    d_qkv_b = d_qkv_b_parts[0] + x_swap(d_qkv_b_parts[1])
    d_qkv_w_recv = x_swap(dot('btd,btshc->sdhc', h_one, d_qkv_all[1]))
    d_qkv_w = dot('btd,btshc->sdhc', h_one, d_qkv_all[0]) + d_qkv_w_recv

    def d_h_one_part(tokens):
        return sum(dot('btshc,sdhc->btd', d_qkv[:, tokens], w_val) for d_qkv, w_val in zip(d_qkv_all, qkv_w_all))

    d_h_one_recv = core_swap(d_h_one_part(second))
    d_h_one = (d_h_one_part(first) + d_h_one_recv).astype(HALF)
    d_emb_ln, d_ln1_scale, d_ln1_bias = ln_one_vjp(d_h_one.astype(WIDE))
    d_emb = (d_x_one.astype(WIDE) + d_emb_ln).astype(HALF)
    d_pos_both = jnp.sum(d_emb, axis=0, dtype=WIDE)
    d_pos = d_pos_both[:n_tok] + x_swap(d_pos_both[n_tok:])
    d_patch_b = jnp.sum(d_pos_both, axis=0)
    d_patch_part = dot('btp,btd->pd', pat, d_emb)

    oth_a = mlp_up(h_two_oa, fc1_w, fc1_b)
    oth_b = mlp_up(h_two_ob, fc1_w, fc1_b)
    d_pre_oth_a = d_up(d_two_oa, oth_a[1], fc2_w)
    d_pre_oth_b = d_up(d_two_ob, oth_b[1], fc2_w)
    d_pres = (d_pre_own_a, d_pre_own_b, d_pre_oth_a, d_pre_oth_b)
    d_fc1_b = sum(jnp.sum(val, axis=(0, 1)) for val in d_pres)
    d_fc1_w = sum(dot('btd,btf->df', h_val, val.astype(HALF)) for h_val, val in zip((h_two_a, h_two_b, h_two_oa, h_two_ob), d_pres))
    d_fc2_w = sum(dot('btf,btd->fd', val[0], d_two) for val, d_two in zip((own_a, own_b, oth_a, oth_b), (d_two_a, d_two_b, d_two_oa, d_two_ob)))
    d_fc2_b = jnp.sum(d_out, axis=(0, 1), dtype=WIDE)

    small = jnp.stack([d_patch_b, d_ln1_scale, d_ln2_scale, d_ln1_bias, d_ln2_bias, d_out_b, d_fc2_b, jnp.zeros_like(d_fc2_b)])
    small = small + core_swap(small)
    small = small + x_swap(small)
    core = lax.axis_index('tp') % 2
    rows = d_patch_part.shape[0] // 2
    mine = lax.dynamic_slice_in_dim(d_patch_part, core * rows, rows, 0)
    theirs = lax.dynamic_slice_in_dim(d_patch_part, (1 - core) * rows, rows, 0)
    mine = mine + core_swap(theirs)
    mine = (mine + x_swap(mine)).astype(HALF)
    theirs = core_swap(mine)
    d_patch_w = jnp.where(core == 0, jnp.concatenate([mine, theirs]), jnp.concatenate([theirs, mine]))

    return (x_two_out, d_patch_w, small[0].astype(HALF), d_pos.astype(HALF), small[1:3].astype(HALF), small[3:5].astype(HALF), d_qkv_w.astype(HALF), d_qkv_b.astype(HALF), d_out_w.astype(HALF), small[5].astype(HALF), d_fc1_w.astype(HALF), d_fc1_b.astype(HALF), d_fc2_w.astype(HALF), small[6].astype(HALF))


def solution(mesh):
    in_specs = (P('dp', 'tp', None), P(), P(), P('tp', None), P(), P(), P(None, None, 'tp', None), P(None, 'tp', None), P('tp', None, None), P(), P(None, 'tp'), P('tp'), P('tp', None), P(), P('dp', 'tp', None))
    out_specs = (P('dp', 'tp', None), P('dp', None), P('dp'), P(('dp', 'tp'), None), P('dp', None), P('dp', None), P('dp', None, 'tp', None), P('dp', 'tp', None), P(('dp', 'tp'), None, None), P('dp'), P('dp', 'tp'), P(('dp', 'tp')), P(('dp', 'tp'), None), P('dp'))
    return jax.shard_map(group_step, mesh=mesh, in_specs=in_specs, out_specs=out_specs, check_vma=False)
```

```python
import jax
import jax.numpy as jnp
from jax import lax
from jax.experimental import pallas as pl
from jax.experimental.pallas import tpu as pltpu
from jax.sharding import PartitionSpec as P

LN_EPS = 1e-6
CORE_PAIRS, X_PAIRS, DIAG_PAIRS = [[(i, i ^ hop) for i in range(4)] for hop in range(1, 4)]
WIDE = jnp.float32
HALF = jnp.bfloat16
LANES = 128
GELU_A = 0.7978845608028654
GELU_B = 0.044715
MLP_TILE = 256


def x_swap(val):
    return lax.ppermute(val, 'tp', X_PAIRS)


def core_swap(val):
    return lax.ppermute(val, 'tp', CORE_PAIRS)


def normalize(x_val):
    centered = x_val - jnp.mean(x_val, axis=-1, keepdims=True)
    row_rstd = lax.rsqrt(jnp.mean(centered * centered, axis=-1, keepdims=True) + LN_EPS)
    return centered * row_rstd, row_rstd


def normalize_back(x_val, scale_f, d_out):
    unit, row_rstd = normalize(x_val)
    d_unit = d_out * scale_f
    inner = d_unit - jnp.mean(d_unit, axis=-1, keepdims=True) - unit * jnp.mean(d_unit * unit, axis=-1, keepdims=True)
    return row_rstd * inner, jnp.sum(d_out * unit, axis=0, keepdims=True), jnp.sum(d_out, axis=0, keepdims=True)


def mm(lhs, rhs):
    return jnp.dot(lhs, rhs, preferred_element_type=WIDE)


def mm_nt(lhs, rhs):
    return lax.dot_general(lhs, rhs, (((1,), (1,)), ((), ())), preferred_element_type=WIDE)


def mm_tn(lhs, rhs):
    return lax.dot_general(lhs, rhs, (((0,), (0,)), ((), ())), preferred_element_type=WIDE)


def run(kernel, grid, in_specs, out_specs, out_shape, flops, scratch=()):
    total = sum(s.size * s.dtype.itemsize for s in jax.tree.leaves(out_shape))
    return pl.pallas_call(
        kernel, grid=(grid,), in_specs=in_specs, out_specs=out_specs, out_shape=out_shape, scratch_shapes=list(scratch),
        cost_estimate=pl.CostEstimate(flops=int(flops), bytes_accessed=2 * total, transcendentals=0),
        compiler_params=pltpu.CompilerParams(dimension_semantics=("arbitrary",)))


def fixed(shape):
    return pl.BlockSpec(shape, lambda i: (0,) * len(shape))


def held(shape):
    return pl.BlockSpec(shape, lambda i: (0,) * len(shape), pipeline_mode=pl.Buffered(1))


def tiled(rows, cols):
    return pl.BlockSpec((rows, cols), lambda i: (i, 0))


STEP = 256


def chunks(size):
    return [slice(col, col + STEP) for col in range(0, size, STEP)]


def first_step(*refs):
    @pl.when(pl.program_id(0) == 0)
    def _():
        for ref in refs:
            ref[...] = jnp.zeros_like(ref)


def shape_of(*dims, dtype=HALF):
    return jax.ShapeDtypeStruct(dims, dtype)


def diag_swap(val):
    return lax.ppermute(val, 'tp', DIAG_PAIRS)


def block(rows, width, at):
    return pl.BlockSpec((rows, width), lambda i: (i, at))


def masks():
    lane = lax.broadcasted_iota(jnp.int32, (1, LANES), 1)
    low = jnp.where(lane < LANES // 2, 1.0, 0.0)
    return low.astype(HALF), (1.0 - low).astype(HALF)


def softmax_cols(keys, query):
    scores = mm_nt(keys, query)
    top = jnp.max(scores, axis=0, keepdims=True)
    weights = jnp.exp((scores - top) * 0.125)
    return weights * (1.0 / jnp.sum(weights, axis=0, keepdims=True))


def split(val, both, axis=0):
    return jnp.concatenate([val * m for m in both], axis=axis)


def rows_of(refs):
    return jnp.concatenate([ref[img] for img in range(refs[0].shape[0]) for ref in refs], axis=0)


def pos_of(ref, dim):
    return jnp.concatenate([ref[0], ref[1][:, :dim - ref.shape[2]]], axis=1).astype(WIDE)


def row_of(ref, first, size):
    used = ref.shape[2] - 512
    parts = [ref[1, first + i:first + i + 1, used:] for i in range(2)]
    return jnp.concatenate(parts, axis=1)[:, :size].astype(WIDE)


def front_kernel(p0_ref, p1_ref, p2_ref, p3_ref, e0_ref, e1_ref, e2_ref, e3_ref,
                 patch_w_ref, patch_b_ref, scale_ref, bias_ref, out_b_ref, w0_ref, w1_ref, w2_ref, w3_ref,
                 emb_ref, qkv_ref, ctx_ref, x_ref, h_ref, pack_ref, acc_ref):
    dim = emb_ref.shape[1]
    width = w0_ref.shape[1] // 4
    both = masks()
    pos = jnp.concatenate([pos_of(ref, dim) for ref in (e0_ref, e1_ref, e2_ref, e3_ref)], axis=0)
    emb = (mm(rows_of((p0_ref, p1_ref, p2_ref, p3_ref)), patch_w_ref[...]) + patch_b_ref[...].astype(WIDE) + pos).astype(HALF)
    emb_ref[...] = emb
    unit, _ = normalize(emb.astype(WIDE))
    h_one = (unit * scale_ref[:1, :].astype(WIDE) + bias_ref[:1, :].astype(WIDE)).astype(HALF)
    pack_ref[:, :dim] = h_one
    for side, w_ref in enumerate((w0_ref, w1_ref, w2_ref, w3_ref)):
        base = 3 * width * side
        bias = row_of((e0_ref, e2_ref, e1_ref, e3_ref)[side], 0, 3 * width)
        for col in range(0, 3 * width, STEP):
            qkv_ref[:, base + col:base + col + STEP] = (mm(h_one, w_ref[:, col:col + STEP]) + bias[:, col:col + STEP]).astype(HALF)
        ctx = []
        for col in range(0, width, LANES):
            query, keys, vals = [qkv_ref[:, base + width * i + col:base + width * i + col + LANES] for i in range(3)]
            probs = jnp.concatenate([softmax_cols(keys, query * m).astype(HALF) for m in both], axis=0)
            ctx.append(mm_tn(split(vals, both), probs).T.astype(HALF))
        ctx = jnp.concatenate(ctx, axis=1)
        to_ref, to = (ctx_ref, width * side) if side < 2 else (pack_ref, 2 * dim + width * (side - 2))
        to_ref[:, to:to + width] = ctx
        part = mm_nt(ctx, w_ref[:, 3 * width:])
        acc_ref[...] = part if side == 0 else acc_ref[...] + part
    x_one = (emb_ref[...].astype(WIDE) + (acc_ref[...] + out_b_ref[...].astype(WIDE))).astype(HALF)
    x_ref[...] = x_one
    unit, _ = normalize(x_one.astype(WIDE))
    h_two = (unit * scale_ref[1:2, :].astype(WIDE) + bias_ref[1:2, :].astype(WIDE)).astype(HALF)
    h_ref[...] = h_two
    pack_ref[:, dim:2 * dim] = h_two


def image_blocks(vals, count=1):
    return [pl.BlockSpec((count,) + val.shape[1:], lambda i: (i, 0, 0)) for val in vals]


def extra_blocks(vals):
    return [pl.BlockSpec((2,) + val.shape[1:], lambda i, at=val.shape[0] // 2 - 1: (at, 0, 0)) for val in vals]


def front(got, patch_w, patch_b, scale, bias, out_b, weights):
    n_own, dim, tile = got[0].shape[0] - 2, patch_w.shape[1], 4 * got[0].shape[1]
    rows = n_own * tile
    outs = [shape_of(rows, dim), shape_of(rows, 3 * dim), shape_of(rows, dim // 2), shape_of(rows, dim), shape_of(rows, dim), shape_of(rows, 2 * dim + dim // 2)]
    vals = (patch_w, patch_b, scale, bias, out_b, *weights)
    return run(front_kernel, n_own, image_blocks(got) + extra_blocks(got) + [held(v.shape) for v in vals], [tiled(tile, o.shape[1]) for o in outs], outs,
               10 * rows * dim * dim, [pltpu.VMEM((tile, dim), WIDE)])(*got, *got, *vals)


def rear_kernel(qkv_ref, dx_ref, emb_ref, p0_ref, p1_ref, p2_ref, p3_ref, scale_ref, w0_ref, w1_ref, w2_ref, w3_ref,
                near_ref, far_ref, patch_ref, pos_ref, sum_ref, qsum_ref, acc_ref):
    first_step(patch_ref, pos_ref, sum_ref, qsum_ref)
    width = w0_ref.shape[1] // 4
    both = masks()
    d_x = dx_ref[...]
    for side, w_ref in enumerate((w0_ref, w1_ref, w2_ref, w3_ref)):
        base = 3 * width * side
        d_ctx_side = mm(d_x, w_ref[:, 3 * width:]).astype(HALF)
        to_ref, to = (near_ref, base) if side < 2 else (far_ref, base - 6 * width)
        for col in range(0, width, LANES):
            query, keys, vals = [qkv_ref[:, base + width * i + col:base + width * i + col + LANES] for i in range(3)]
            d_ctx = d_ctx_side[:, col:col + LANES]
            probs_h, d_scores = [], []
            for m in both:
                probs = softmax_cols(keys, query * m)
                d_probs = mm_nt(vals, d_ctx * m).astype(HALF).astype(WIDE)
                inner = jnp.sum(d_probs * probs, axis=0, keepdims=True)
                d_scores.append((probs * (d_probs - inner) * 0.125).astype(HALF))
                probs_h.append(probs.astype(HALF))
            d_query = mm_tn(split(keys, both), jnp.concatenate(d_scores, axis=0)).T
            d_keys = mm(jnp.concatenate(d_scores, axis=1), split(query, both))
            d_vals = mm(jnp.concatenate(probs_h, axis=1), split(d_ctx, both))
            for i, val in enumerate((d_query, d_keys, d_vals)):
                val_h = val.astype(HALF)
                at = width * i + col
                to_ref[:, to + at:to + at + LANES] = val_h
                qsum_ref[:, base + at:base + at + LANES] += jnp.sum(val_h.astype(WIDE), axis=0, keepdims=True)
        part = mm_nt(to_ref[:, to:to + 3 * width], w_ref[:, :3 * width])
        acc_ref[...] = part if side == 0 else acc_ref[...] + part
    d_h = acc_ref[...].astype(HALF).astype(WIDE)
    d_ln, d_scale, d_bias = normalize_back(emb_ref[...].astype(WIDE), scale_ref[:1, :].astype(WIDE), d_h)
    d_emb = (d_x.astype(WIDE) + d_ln).astype(HALF)
    pos_ref[...] += d_emb.astype(WIDE)
    sum_ref[...] += jnp.concatenate([d_scale, d_bias, jnp.zeros((6, d_emb.shape[1]), WIDE)], axis=0)
    pat = rows_of((p0_ref, p1_ref, p2_ref, p3_ref))
    for rows in chunks(patch_ref.shape[0]):
        patch_ref[rows, :] += mm_tn(pat[:, rows], d_emb)


def rear(qkv, d_x, emb, got, scale, weights):
    rows, dim, tile = emb.shape[0], emb.shape[1], 256
    outs = [shape_of(rows, 3 * dim // 2)] * 2 + [shape_of(got[0].shape[2], dim, dtype=WIDE), shape_of(tile, dim, dtype=WIDE), shape_of(8, dim, dtype=WIDE), shape_of(1, 3 * dim, dtype=WIDE)]
    specs = [tiled(tile, 3 * dim), tiled(tile, dim), tiled(tile, dim)] + image_blocks(got) + [held(scale.shape)] + [held(w.shape) for w in weights]
    return run(rear_kernel, rows // tile, specs, [tiled(tile, 3 * dim // 2)] * 2 + [fixed(o.shape) for o in outs[2:]], outs,
               16 * rows * dim * dim, [pltpu.VMEM((tile, dim), WIDE)])(qkv, d_x, emb, *got, scale, *weights)


def weight_spec(weight):
    val, at = weight
    if val.ndim == 2:
        return held(val.shape)
    return pl.BlockSpec((val.shape[0], 1) + val.shape[2:], lambda i: (0, at, 0, 0), pipeline_mode=pl.Buffered(1))


def w_cols(ref, cols):
    if len(ref.shape) == 2:
        return ref[:, cols]
    return ref[:, 0, :, cols].reshape(ref.shape[0] * ref.shape[2], STEP)


def w_rows(ref, rows):
    if len(ref.shape) == 2:
        return ref[rows, :]
    return ref[rows.start // STEP, 0]


def gelu_both(pre, d_hidden):
    d_hidden = d_hidden.astype(HALF).astype(WIDE)
    square = pre * pre
    bent = jnp.tanh(pre * (GELU_A + (GELU_A * GELU_B) * square))
    cdf = 0.5 + 0.5 * bent
    slope = cdf + pre * (0.5 - 0.5 * bent * bent) * (GELU_A + (3.0 * GELU_A * GELU_B) * square)
    return (pre * cdf).astype(HALF), d_hidden * slope


def up(h_val, d_val, w1_ref, bias, w2_ref, store):
    waiting = None
    for cols in chunks(bias.shape[1]):
        ready = (cols, mm(h_val, w_cols(w1_ref, cols)), mm_nt(d_val, w_rows(w2_ref, cols)))
        if waiting is not None:
            store(waiting[0], *gelu_both(waiting[1] + bias[:, waiting[0]], waiting[2]))
        waiting = ready
    store(waiting[0], *gelu_both(waiting[1] + bias[:, waiting[0]], waiting[2]))


def mlp_kernel(h_ref, x_ref, b2_ref, scale_ref, *refs):
    d_refs, w1_refs, b1_refs, w2_refs = refs[:4], refs[4:8], refs[8:12], refs[12:16]
    own_ref, pack_ref, out_ref, dx_ref, sum_ref, bsum_ref, g_ref, p_ref, acc_ref, dacc_ref = refs[16:]
    first_step(sum_ref, bsum_ref)
    dim = h_ref.shape[1]
    cols_n = g_ref.shape[1]
    d_two = rows_of(d_refs)
    pack_ref[:, 2 * dim:] = d_two
    for side in range(4):
        def store(cols, hidden, d_pre):
            d_pre_h = d_pre.astype(HALF)
            g_ref[:, cols] = hidden
            p_ref[:, cols] = d_pre_h
            shifted = slice(cols_n + cols.start, cols_n + cols.stop)
            if side == 0:
                own_ref[:, cols] = hidden
                own_ref[:, shifted] = d_pre_h
            if side == 2:
                pack_ref[:, cols] = hidden
                pack_ref[:, shifted] = d_pre_h
            if side in (0, 2):
                bsum_ref[side // 2:side // 2 + 1, cols] += jnp.sum(d_pre, axis=0, keepdims=True)

        up(h_ref[...], d_two, w1_refs[side], row_of(b1_refs[side], 2, cols_n), w2_refs[side], store)
        for cols in chunks(dim):
            total = mm(g_ref[...], w_cols(w2_refs[side], cols))
            d_total = mm_nt(p_ref[...], w_rows(w1_refs[side], cols))
            acc_ref[:, cols] = total if side == 0 else acc_ref[:, cols] + total
            dacc_ref[:, cols] = d_total if side == 0 else dacc_ref[:, cols] + d_total
    out_ref[...] = (x_ref[...].astype(WIDE) + (acc_ref[...] + b2_ref[...].astype(WIDE))).astype(HALF)
    d_h = dacc_ref[...].astype(HALF).astype(WIDE)
    d_ln, d_scale, d_bias = normalize_back(x_ref[...].astype(WIDE), scale_ref[1:2, :].astype(WIDE), d_h)
    d_x = (pack_ref[:, 2 * dim:].astype(WIDE) + d_ln).astype(HALF)
    dx_ref[...] = d_x
    sum_ref[...] += jnp.concatenate([d_scale, d_bias, jnp.sum(d_x.astype(WIDE), axis=0, keepdims=True), jnp.zeros((5, dim), WIDE)], axis=0)


def mlp(h_val, d_blocks, x_val, b2, scale, w1s, biases, w2s):
    rows, dim, cols, tile = h_val.shape[0], h_val.shape[1], w2s[0][0].shape[0], MLP_TILE
    specs = [tiled(tile, dim)] * 2 + [held(b2.shape), held(scale.shape)] + image_blocks(d_blocks, tile * d_blocks[0].shape[0] // rows) + [weight_spec(w) for w in w1s] + extra_blocks(biases) + [weight_spec(w) for w in w2s]
    outs = [shape_of(rows, 2 * cols), shape_of(rows, 3 * dim), shape_of(rows, dim), shape_of(rows, dim), shape_of(8, dim, dtype=WIDE), shape_of(8, cols, dtype=WIDE)]
    scratch = [pltpu.VMEM((tile, cols), HALF)] * 2 + [pltpu.VMEM((tile, dim), WIDE)] * 2
    return run(mlp_kernel, rows // tile, specs, [tiled(tile, o.shape[1]) for o in outs[:4]] + [fixed(o.shape) for o in outs[4:]], outs,
               32 * rows * dim * cols, scratch)(h_val, x_val, b2, scale, *d_blocks, *[w[0] for w in w1s], *biases, *[w[0] for w in w2s])


def grad_kernel(la_ref, lb_ref, ra_ref, rb_ref, *out_refs):
    first_step(*out_refs)
    width = out_refs[0].shape[1]
    for rows in chunks(out_refs[0].shape[0]):
        for at, out_ref in enumerate(out_refs):
            cols = slice(width * at, width * (at + 1))
            out_ref[rows, :] += mm_tn(la_ref[:, rows], ra_ref[:, cols]) + mm_tn(lb_ref[:, rows], rb_ref[:, cols])


def grad(ops, count):
    (lhs, dim, _), _, (_, size, _), _ = ops
    rows, tile, width = lhs.shape[0], 512, size // count
    out = shape_of(dim, width, dtype=WIDE)
    return run(grad_kernel, rows // tile, [block(tile, size, at) for _, size, at in ops], [fixed(out.shape)] * count, [out] * count,
               4 * count * rows * dim * width)(*[val for val, _, _ in ops])


def grad_mlp_kernel(ha_ref, ga_ref, da_ref, hb_ref, gb_ref, db_ref, hx_ref, dx_ref, hd_ref, dd_ref, w1_ref, b1_ref, w2_ref,
                    out1_ref, out2_ref, bsum_ref, acc1_ref, acc2_ref, g_ref, p_ref):
    first_step(bsum_ref, acc1_ref, acc2_ref)
    cols_n = w1_ref.shape[1]
    for at, (h_ref, d_ref) in enumerate(((hx_ref, dx_ref), (hd_ref, dd_ref))):
        def store(cols, hidden, d_pre):
            g_ref[at, :, cols] = hidden
            p_ref[at, :, cols] = d_pre.astype(HALF)
            bsum_ref[:, cols] += jnp.sum(d_pre, axis=0, keepdims=True)

        up(h_ref[...], d_ref[...], w1_ref, b1_ref[...].astype(WIDE), w2_ref, store)
    for rows in chunks(acc1_ref.shape[0]):
        acc1_ref[rows, :] += mm_tn(ha_ref[:, rows], ga_ref[:, cols_n:]) + mm_tn(hb_ref[:, rows], gb_ref[:, cols_n:]) + mm_tn(hx_ref[:, rows], p_ref[0]) + mm_tn(hd_ref[:, rows], p_ref[1])
    for rows in chunks(acc2_ref.shape[0]):
        acc2_ref[rows, :] += mm_tn(ga_ref[:, rows], da_ref[...]) + mm_tn(gb_ref[:, rows], db_ref[...]) + mm_tn(g_ref[0, :, rows], dx_ref[...]) + mm_tn(g_ref[1, :, rows], dd_ref[...])

    @pl.when(pl.program_id(0) == pl.num_programs(0) - 1)
    def _():
        out1_ref[...] = acc1_ref[...].astype(HALF)
        out2_ref[...] = acc2_ref[...].astype(HALF)


def grad_mlp(ops, w1, b1, w2):
    rows, (dim, cols), tile = ops[0][0].shape[0], w1.shape, 256
    outs = [shape_of(dim, cols), shape_of(cols, dim), shape_of(1, cols, dtype=WIDE)]
    scratch = [pltpu.VMEM((dim, cols), WIDE), pltpu.VMEM((cols, dim), WIDE)] + [pltpu.VMEM((2, tile, cols), HALF)] * 2
    return run(grad_mlp_kernel, rows // tile, [block(tile, width, at) for _, width, at in ops] + [held(w1.shape), held(b1.shape), held(w2.shape)],
               [fixed(o.shape) for o in outs], outs, 24 * rows * dim * cols, scratch)(*[val for val, _, _ in ops], w1, b1, w2)


def gather_pieces(piece):
    group = lax.axis_index('dp')
    pieces = [(x_swap(piece), group)]
    for hop, at in enumerate((group + 1 - 2 * (group % 2), (group + 2) % 4, 3 - group), 1):
        pieces.append((lax.ppermute(pieces[0][0], 'dp', [(i, i ^ hop) for i in range(4)]), at))
    return pieces


def after(vals, done):
    return lax.optimization_barrier((vals, done))[0]


def group_step(patches, patch_w, patch_b, pos_emb, ln_scale, ln_bias, qkv_w, qkv_b, out_w, out_b, fc1_w, fc1_b, fc2_w, fc2_b, d_out):
    n_img, n_tok, patch_dim = patches.shape
    dim = patch_w.shape[1]
    n_own = n_img // 4
    rows = n_own * 4 * n_tok
    cols = fc1_w.shape[1]
    group, me = lax.axis_index('dp'), lax.axis_index('tp')
    core = me % 2
    core_set = me + 1 - 2 * core
    sets = (me, core_set, (me + 2) % 4, (core_set + 2) % 4)

    def images(val, which):
        return lax.dynamic_slice_in_dim(val, sets[which] * n_own, n_own, 0)

    def quarter(val):
        part = val.shape[0] // 4
        return lax.dynamic_slice_in_dim(val, group * part, part, 0)

    row = lambda val: val.reshape(1, val.shape[-1])

    heads = qkv_w.shape[2] * qkv_w.shape[3]
    attn_w = jnp.concatenate([jnp.swapaxes(qkv_w, 0, 1).reshape(dim, 3 * heads), out_w.reshape(heads, dim).T], axis=1)
    attn_pieces = gather_pieces(quarter(attn_w))
    flat = jnp.concatenate([qkv_b.reshape(3 * heads), jnp.zeros((1024 - 3 * heads,), HALF), fc1_b]).reshape(4, 512)
    beside = jnp.concatenate([pos_emb[:, patch_dim:], jnp.pad(flat, ((0, n_tok - 4), (0, 0)))], axis=1)
    extra = jnp.stack([pos_emb[:, :patch_dim], beside])
    with_extra = lambda which: jnp.concatenate([images(patches, which), extra], axis=0)
    got = (with_extra(0), core_swap(with_extra(1)), x_swap(with_extra(2)), diag_swap(with_extra(3)))
    mlp_pieces = gather_pieces(jnp.stack([quarter(fc1_w), quarter(fc2_w)]))
    d_blocks = (images(d_out, 0), core_swap(images(d_out, 1)), x_swap(images(d_out, 2)), diag_swap(images(d_out, 3)))
    attn_c = core_swap(attn_w)
    fc1_c, fc2_c = core_swap(fc1_w), core_swap(fc2_w)

    attn_x = jnp.zeros_like(attn_w)
    for val, at in attn_pieces:
        attn_x = lax.dynamic_update_slice(attn_x, val, (at * (dim // 4), 0))
    attn_d = core_swap(attn_x)
    mlp_x = jnp.zeros((4, 2, dim // 4, cols), HALF)
    for val, at in mlp_pieces:
        mlp_x = lax.dynamic_update_slice(mlp_x, val[None], (at, 0, 0, 0))
    mlp_d = core_swap(mlp_x)
    attn_ws = (attn_w, attn_x, attn_c, attn_d)

    emb, qkv, ctx, x_one, h_two, pack_f = front(got, patch_w, row(patch_b), ln_scale, ln_bias, row(out_b), attn_ws)
    h_two_x = x_swap(h_two)
    pack_f_c = core_swap(pack_f)
    h_two_d = core_swap(h_two_x)

    w1s, w2s = ((fc1_w, 0), (mlp_x, 0), (fc1_c, 0), (mlp_d, 0)), ((fc2_w, 0), (mlp_x, 1), (fc2_c, 0), (mlp_d, 1))
    own_gp, pack_m, x_two, d_x, sums_two, b_sums = mlp(h_two, d_blocks, x_one, row(fc2_b), ln_scale, w1s, (got[0], got[2], got[1], got[3]), w2s)
    pack_m_c = core_swap(pack_m)
    x_blocks = x_two.reshape(n_own, 4, n_tok, dim)
    x_parts = (x_blocks[:, 0], core_swap(x_blocks[:, 1]), x_swap(x_blocks[:, 2]), diag_swap(x_blocks[:, 3]))
    d_x_c = core_swap(d_x)
    d_o_own, d_o_x = grad(((d_x, dim, 0), (d_x_c, dim, 0), (ctx, 2 * heads, 0), (pack_f_c, 2 * heads, 4)), 2)
    d_o_recv = x_swap(d_o_x)
    d_near, d_far, d_patch_part, d_pos_all, sums_one, d_qkv_sum = rear(qkv, d_x, emb, got, ln_scale, attn_ws)
    d_far_c = core_swap(d_far)
    third = 3 * heads
    d_qkv_x, = grad(((pack_f, dim, 0), (pack_f_c, dim, 0), (d_near, third, 1), (d_far_c, third, 1)), 1)
    d_qkv_recv = x_swap(d_qkv_x)
    d_qkv_own, = grad(((pack_f, dim, 0), (pack_f_c, dim, 0), (d_near, third, 0), (d_far_c, third, 0)), 1)

    def in_order(flip, low, high):
        return jnp.where(flip == 0, jnp.concatenate([low, high], axis=0), jnp.concatenate([high, low], axis=0))

    x_parts = after(x_parts, d_qkv_x)
    x_two_out = in_order(me // 2, in_order(core, x_parts[0], x_parts[1]), in_order(core, x_parts[2], x_parts[3]))

    d_parts = (x_swap(images(d_out, 0)), diag_swap(images(d_out, 1)), images(d_out, 2), core_swap(images(d_out, 3)))
    d_oth = jnp.concatenate(after(d_parts, d_qkv_x), axis=1).reshape(rows, dim)
    d_oth_d = core_swap(d_oth)
    d_fc1_w, d_fc2_w, sum_other = grad_mlp((
        (h_two, dim, 0), (own_gp, 2 * cols, 0), (pack_m, dim, 2), (pack_f_c, dim, 1), (pack_m_c, 2 * cols, 0), (pack_m_c, dim, 2),
        (h_two_x, dim, 0), (d_oth, dim, 0), (h_two_d, dim, 0), (d_oth_d, dim, 0)), fc1_w, row(fc1_b), fc2_w)
    d_fc2_b = jnp.sum(d_out, axis=(0, 1), dtype=WIDE)

    half_rows = patch_dim // 2
    mine = lax.dynamic_slice_in_dim(d_patch_part, core * half_rows, half_rows, 0)
    theirs = lax.dynamic_slice_in_dim(d_patch_part, (1 - core) * half_rows, half_rows, 0)
    mine = mine + core_swap(theirs)
    mine = (mine + x_swap(mine)).astype(HALF)
    theirs = core_swap(mine)
    d_patch_w = jnp.where(core == 0, jnp.concatenate([mine, theirs]), jnp.concatenate([theirs, mine]))

    d_pos_all, d_qkv_sum, sums_one = after((d_pos_all, d_qkv_sum, sums_one), d_qkv_x)
    d_patch_b = jnp.sum(d_pos_all, axis=0, keepdims=True)
    small = jnp.concatenate([sums_one[:1], sums_two[:1], sums_one[1:2], sums_two[1:2], sums_two[2:3], d_patch_b, row(d_fc2_b)], axis=0)
    wide_row = lambda side: jnp.pad(d_qkv_sum[:, 3 * heads * side:3 * heads * (side + 1)], ((0, 0), (0, dim - 3 * heads)))
    pos_block = lambda at: d_pos_all[at * n_tok:(at + 1) * n_tok]
    from_core = core_swap(jnp.concatenate([pos_block(1), pos_block(3), small, wide_row(2), wide_row(3), b_sums[1:2]], axis=0))
    mine_sum = jnp.concatenate([pos_block(0), pos_block(2), small, wide_row(0), wide_row(1), b_sums[:1]], axis=0) + from_core
    d_fc1_b = mine_sum[2 * n_tok + 9] + sum_other[0]
    small = mine_sum[2 * n_tok:2 * n_tok + 7]
    from_x = x_swap(jnp.concatenate([mine_sum[n_tok:2 * n_tok], small, mine_sum[2 * n_tok + 8:2 * n_tok + 9]], axis=0))
    total = (jnp.concatenate([mine_sum[:n_tok], small, mine_sum[2 * n_tok + 7:2 * n_tok + 8]], axis=0) + from_x).astype(HALF)
    d_pos, small, d_qkv_b = total[:n_tok], total[n_tok:n_tok + 7], total[n_tok + 7, :3 * heads]

    d_qkv_w = jnp.swapaxes((d_qkv_own + d_qkv_recv).astype(HALF).reshape((dim,) + qkv_b.shape), 0, 1)
    d_out_w = (d_o_own + d_o_recv).astype(HALF).T.reshape(out_w.shape)
    return (x_two_out, d_patch_w, small[5], d_pos, small[:2], small[2:4], d_qkv_w, d_qkv_b.reshape(qkv_b.shape), d_out_w, small[4], d_fc1_w, d_fc1_b.astype(HALF), d_fc2_w, small[6])


def solution(mesh):
    in_specs = (P('dp', 'tp'), P(), P(), P('tp'), P(), P(), P(None, None, 'tp'), P(None, 'tp'), P('tp'), P(), P(None, 'tp'), P('tp'), P('tp'), P(), P('dp', 'tp'))
    out_specs = (P('dp', 'tp'), P('dp'), P('dp'), P(('dp', 'tp')), P('dp'), P('dp'), P('dp', None, 'tp'), P('dp', 'tp'), P(('dp', 'tp')), P('dp'), P('dp', 'tp'), P(('dp', 'tp')), P(('dp', 'tp')), P('dp'))
    return jax.shard_map(group_step, mesh=mesh, in_specs=in_specs, out_specs=out_specs, check_vma=False)
```

```python
import jax
import jax.numpy as jnp
from jax import lax
from jax.experimental import pallas as pl
from jax.experimental.pallas import tpu as pltpu
from jax.sharding import PartitionSpec as P

LN_EPS = 1e-6
CORE_PAIRS, X_PAIRS, DIAG_PAIRS = [[(i, i ^ hop) for i in range(4)] for hop in range(1, 4)]
WIDE = jnp.float32
HALF = jnp.bfloat16
LANES = 128
GELU_A = 0.7978845608028654
GELU_B = 0.044715


def x_swap(val):
    return lax.ppermute(val, 'tp', X_PAIRS)


def core_swap(val):
    return lax.ppermute(val, 'tp', CORE_PAIRS)


def normalize(x_val):
    centered = x_val - jnp.mean(x_val, axis=-1, keepdims=True)
    row_rstd = lax.rsqrt(jnp.mean(centered * centered, axis=-1, keepdims=True) + LN_EPS)
    return centered * row_rstd, row_rstd


def normalize_back(x_val, scale_f, d_out):
    unit, row_rstd = normalize(x_val)
    d_unit = d_out * scale_f
    inner = d_unit - jnp.mean(d_unit, axis=-1, keepdims=True) - unit * jnp.mean(d_unit * unit, axis=-1, keepdims=True)
    return row_rstd * inner, jnp.sum(d_out * unit, axis=0, keepdims=True), jnp.sum(d_out, axis=0, keepdims=True)


def mm(lhs, rhs):
    return jnp.dot(lhs, rhs, preferred_element_type=WIDE)


def mm_nt(lhs, rhs):
    return lax.dot_general(lhs, rhs, (((1,), (1,)), ((), ())), preferred_element_type=WIDE)


def mm_tn(lhs, rhs):
    return lax.dot_general(lhs, rhs, (((0,), (0,)), ((), ())), preferred_element_type=WIDE)


def run(kernel, grid, in_specs, out_specs, out_shape, flops, scratch=()):
    total = sum(s.size * s.dtype.itemsize for s in jax.tree.leaves(out_shape))
    return pl.pallas_call(
        kernel, grid=(grid,), in_specs=in_specs, out_specs=out_specs, out_shape=out_shape, scratch_shapes=list(scratch),
        cost_estimate=pl.CostEstimate(flops=int(flops), bytes_accessed=2 * total, transcendentals=0),
        compiler_params=pltpu.CompilerParams(dimension_semantics=("arbitrary",)))


def fixed(shape):
    return pl.BlockSpec(shape, lambda i: (0,) * len(shape))


def held(shape):
    return pl.BlockSpec(shape, lambda i: (0,) * len(shape), pipeline_mode=pl.Buffered(1))


def tiled(rows, cols):
    return pl.BlockSpec((rows, cols), lambda i: (i, 0))


STEP = 256


def chunks(size):
    return [slice(col, col + STEP) for col in range(0, size, STEP)]


def first_step(*refs):
    @pl.when(pl.program_id(0) == 0)
    def _():
        for ref in refs:
            ref[...] = jnp.zeros_like(ref)


def shape_of(*dims, dtype=HALF):
    return jax.ShapeDtypeStruct(dims, dtype)


def diag_swap(val):
    return lax.ppermute(val, 'tp', DIAG_PAIRS)


def block(rows, width, at):
    return pl.BlockSpec((rows, width), lambda i: (i, at))


def masks():
    lane = lax.broadcasted_iota(jnp.int32, (1, LANES), 1)
    low = jnp.where(lane < LANES // 2, 1.0, 0.0)
    return low.astype(HALF), (1.0 - low).astype(HALF)


def softmax_cols(keys, query):
    scores = mm_nt(keys, query)
    top = jnp.max(scores, axis=0, keepdims=True)
    weights = jnp.exp((scores - top) * 0.125)
    return weights * (1.0 / jnp.sum(weights, axis=0, keepdims=True))


def split(val, both, axis=0):
    return jnp.concatenate([val * m for m in both], axis=axis)


def rows_of(refs):
    return jnp.concatenate([ref[img] for img in range(refs[0].shape[0]) for ref in refs], axis=0)


def pos_of(ref, dim):
    return jnp.concatenate([ref[0], ref[1][:, :dim - ref.shape[2]]], axis=1).astype(WIDE)


def row_of(ref, first, size):
    used = ref.shape[2] - 512
    parts = [ref[1, first + i:first + i + 1, used:] for i in range(2)]
    return jnp.concatenate(parts, axis=1)[:, :size].astype(WIDE)


def front_kernel(p0_ref, p1_ref, p2_ref, p3_ref, e0_ref, e1_ref, e2_ref, e3_ref,
                 patch_w_ref, patch_b_ref, scale_ref, bias_ref, out_b_ref, w0_ref, w1_ref, w2_ref, w3_ref,
                 emb_ref, qkv_ref, ctx_ref, x_ref, h_ref, pack_ref, acc_ref):
    dim = emb_ref.shape[1]
    width = w0_ref.shape[1] // 4
    both = masks()
    pos = jnp.concatenate([pos_of(ref, dim) for ref in (e0_ref, e1_ref, e2_ref, e3_ref)], axis=0)
    emb = (mm(rows_of((p0_ref, p1_ref, p2_ref, p3_ref)), patch_w_ref[...]) + patch_b_ref[...].astype(WIDE) + pos).astype(HALF)
    emb_ref[...] = emb
    unit, _ = normalize(emb.astype(WIDE))
    h_one = (unit * scale_ref[:1, :].astype(WIDE) + bias_ref[:1, :].astype(WIDE)).astype(HALF)
    pack_ref[:, :dim] = h_one
    for side, w_ref in enumerate((w0_ref, w1_ref, w2_ref, w3_ref)):
        base = 3 * width * side
        bias = row_of((e0_ref, e2_ref, e1_ref, e3_ref)[side], 0, 3 * width)
        for col in range(0, 3 * width, STEP):
            qkv_ref[:, base + col:base + col + STEP] = (mm(h_one, w_ref[:, col:col + STEP]) + bias[:, col:col + STEP]).astype(HALF)
        ctx = []
        for col in range(0, width, LANES):
            query, keys, vals = [qkv_ref[:, base + width * i + col:base + width * i + col + LANES] for i in range(3)]
            probs = jnp.concatenate([softmax_cols(keys, query * m).astype(HALF) for m in both], axis=0)
            ctx.append(mm_tn(split(vals, both), probs).T.astype(HALF))
        ctx = jnp.concatenate(ctx, axis=1)
        to_ref, to = (ctx_ref, width * side) if side < 2 else (pack_ref, 2 * dim + width * (side - 2))
        to_ref[:, to:to + width] = ctx
        part = mm_nt(ctx, w_ref[:, 3 * width:])
        acc_ref[...] = part if side == 0 else acc_ref[...] + part
    x_one = (emb_ref[...].astype(WIDE) + (acc_ref[...] + out_b_ref[...].astype(WIDE))).astype(HALF)
    x_ref[...] = x_one
    unit, _ = normalize(x_one.astype(WIDE))
    h_two = (unit * scale_ref[1:2, :].astype(WIDE) + bias_ref[1:2, :].astype(WIDE)).astype(HALF)
    h_ref[...] = h_two
    pack_ref[:, dim:2 * dim] = h_two


def image_blocks(vals, count=1):
    return [pl.BlockSpec((count,) + val.shape[1:], lambda i: (i, 0, 0)) for val in vals]


def extra_blocks(vals):
    return [pl.BlockSpec((2,) + val.shape[1:], lambda i, at=val.shape[0] // 2 - 1: (at, 0, 0)) for val in vals]


def front(got, patch_w, patch_b, scale, bias, out_b, weights):
    n_own, dim, tile = got[0].shape[0] - 2, patch_w.shape[1], 4 * got[0].shape[1]
    rows = n_own * tile
    outs = [shape_of(rows, dim), shape_of(rows, 3 * dim), shape_of(rows, dim // 2), shape_of(rows, dim), shape_of(rows, dim), shape_of(rows, 2 * dim + dim // 2)]
    vals = (patch_w, patch_b, scale, bias, out_b, *weights)
    return run(front_kernel, n_own, image_blocks(got) + extra_blocks(got) + [held(v.shape) for v in vals], [tiled(tile, o.shape[1]) for o in outs], outs,
               10 * rows * dim * dim, [pltpu.VMEM((tile, dim), WIDE)])(*got, *got, *vals)


def rear_kernel(qkv_ref, dx_ref, emb_ref, p0_ref, p1_ref, p2_ref, p3_ref, scale_ref, w0_ref, w1_ref, w2_ref, w3_ref,
                near_ref, far_ref, patch_ref, pos_ref, sum_ref, qsum_ref, acc_ref):
    first_step(patch_ref, pos_ref, sum_ref, qsum_ref)
    width = w0_ref.shape[1] // 4
    both = masks()
    d_x = dx_ref[...]
    for side, w_ref in enumerate((w0_ref, w1_ref, w2_ref, w3_ref)):
        base = 3 * width * side
        d_ctx_side = mm(d_x, w_ref[:, 3 * width:]).astype(HALF)
        to_ref, to = (near_ref, base) if side < 2 else (far_ref, base - 6 * width)
        for col in range(0, width, LANES):
            query, keys, vals = [qkv_ref[:, base + width * i + col:base + width * i + col + LANES] for i in range(3)]
            d_ctx = d_ctx_side[:, col:col + LANES]
            probs_h, d_scores = [], []
            for m in both:
                probs = softmax_cols(keys, query * m)
                d_probs = mm_nt(vals, d_ctx * m).astype(HALF).astype(WIDE)
                inner = jnp.sum(d_probs * probs, axis=0, keepdims=True)
                d_scores.append((probs * (d_probs - inner) * 0.125).astype(HALF))
                probs_h.append(probs.astype(HALF))
            d_query = mm_tn(split(keys, both), jnp.concatenate(d_scores, axis=0)).T
            d_keys = mm(jnp.concatenate(d_scores, axis=1), split(query, both))
            d_vals = mm(jnp.concatenate(probs_h, axis=1), split(d_ctx, both))
            for i, val in enumerate((d_query, d_keys, d_vals)):
                val_h = val.astype(HALF)
                at = width * i + col
                to_ref[:, to + at:to + at + LANES] = val_h
                qsum_ref[:, base + at:base + at + LANES] += jnp.sum(val_h.astype(WIDE), axis=0, keepdims=True)
        part = mm_nt(to_ref[:, to:to + 3 * width], w_ref[:, :3 * width])
        acc_ref[...] = part if side == 0 else acc_ref[...] + part
    d_h = acc_ref[...].astype(HALF).astype(WIDE)
    d_ln, d_scale, d_bias = normalize_back(emb_ref[...].astype(WIDE), scale_ref[:1, :].astype(WIDE), d_h)
    d_emb = (d_x.astype(WIDE) + d_ln).astype(HALF)
    pos_ref[...] += d_emb.astype(WIDE)
    sum_ref[...] += jnp.concatenate([d_scale, d_bias, jnp.zeros((6, d_emb.shape[1]), WIDE)], axis=0)
    pat = rows_of((p0_ref, p1_ref, p2_ref, p3_ref))
    for rows in chunks(patch_ref.shape[0]):
        patch_ref[rows, :] += mm_tn(pat[:, rows], d_emb)


def rear(qkv, d_x, emb, got, scale, weights):
    rows, dim, tile = emb.shape[0], emb.shape[1], 256
    outs = [shape_of(rows, 3 * dim // 2)] * 2 + [shape_of(got[0].shape[2], dim, dtype=WIDE), shape_of(tile, dim, dtype=WIDE), shape_of(8, dim, dtype=WIDE), shape_of(1, 3 * dim, dtype=WIDE)]
    specs = [tiled(tile, 3 * dim), tiled(tile, dim), tiled(tile, dim)] + image_blocks(got) + [held(scale.shape)] + [held(w.shape) for w in weights]
    return run(rear_kernel, rows // tile, specs, [tiled(tile, 3 * dim // 2)] * 2 + [fixed(o.shape) for o in outs[2:]], outs,
               16 * rows * dim * dim, [pltpu.VMEM((tile, dim), WIDE)])(qkv, d_x, emb, *got, scale, *weights)


def gelu_both(pre, d_hidden):
    d_hidden = d_hidden.astype(HALF).astype(WIDE)
    square = pre * pre
    bent = jnp.tanh(pre * (GELU_A + (GELU_A * GELU_B) * square))
    cdf = 0.5 + 0.5 * bent
    slope = cdf + pre * (0.5 - 0.5 * bent * bent) * (GELU_A + (3.0 * GELU_A * GELU_B) * square)
    return (pre * cdf).astype(HALF), d_hidden * slope


def up(h_val, d_val, w1_cols, bias, w2_rows, store):
    waiting = None
    for cols in chunks(bias.shape[1]):
        ready = (cols, mm(h_val, w1_cols(cols)), mm_nt(d_val, w2_rows(cols)))
        if waiting is not None:
            store(waiting[0], *gelu_both(waiting[1] + bias[:, waiting[0]], waiting[2]))
        waiting = ready
    store(waiting[0], *gelu_both(waiting[1] + bias[:, waiting[0]], waiting[2]))


def mlp_kernel(h_ref, x_ref, b2_ref, scale_ref, d0_ref, d1_ref, d2_ref, d3_ref, *refs):
    b_refs, near_refs, x_refs, diag_refs = [refs[i:i + 4] for i in range(0, 16, 4)]
    o0_ref, o1_ref, o2_ref, o3_ref, own_ref, pack_ref, dx_ref, sum_ref, bsum_ref, g_ref, p_ref, acc_ref, dacc_ref, w_ref, sem = refs[16:]
    first_step(sum_ref, bsum_ref)
    dim = h_ref.shape[1]
    cols_n = g_ref.shape[1]
    group = lax.axis_index('dp')
    spots = (group, group + 1 - 2 * (group % 2), (group + 2) % 4, 3 - group)

    def copies(side):
        if side % 2:
            moves = [(ref, w_ref.at[side, at]) for ref, at in zip(diag_refs if side > 1 else x_refs, spots)]
        else:
            moves = [(near_refs[side + which], w_ref.at[side, :, which]) for which in range(2)]
        return [pltpu.make_async_copy(*move, sem.at[side, k]) for k, move in enumerate(moves)]

    @pl.when(pl.program_id(0) == 0)
    def _():
        pending = [copy for side in range(4) for copy in copies(side)]
        for copy in pending:
            copy.start()
        for copy in pending:
            copy.wait()

    d_two = rows_of((d0_ref, d1_ref, d2_ref, d3_ref))
    pack_ref[:, 2 * dim:] = d_two
    for side in range(4):
        def w1_cols(cols):
            return w_ref[side, :, 0, :, cols].reshape(dim, STEP)

        def w2_cols(cols):
            return w_ref[side, :, 1, :, cols].reshape(cols_n, STEP)

        def w1_rows(rows):
            return w_ref[side, rows.start // STEP, 0]

        def w2_rows(rows):
            return w_ref[side, rows.start // STEP, 1]

        def store(cols, hidden, d_pre):
            d_pre_h = d_pre.astype(HALF)
            g_ref[:, cols] = hidden
            p_ref[:, cols] = d_pre_h
            if side % 2 == 0:
                to_ref = pack_ref if side else own_ref
                to_ref[:, cols] = hidden
                to_ref[:, cols_n + cols.start:cols_n + cols.stop] = d_pre_h
                bsum_ref[side // 2:side // 2 + 1, cols] += jnp.sum(d_pre, axis=0, keepdims=True)

        up(h_ref[...], d_two, w1_cols, row_of(b_refs[side], 2, cols_n), w2_rows, store)
        for cols in chunks(dim):
            total = mm(g_ref[...], w2_cols(cols))
            d_total = mm_nt(p_ref[...], w1_rows(cols))
            acc_ref[:, cols] = acc_ref[:, cols] + total if side else total
            dacc_ref[:, cols] = dacc_ref[:, cols] + d_total if side else d_total
    x_two = (x_ref[...].astype(WIDE) + (acc_ref[...] + b2_ref[...].astype(WIDE))).astype(HALF)
    for k, ref in enumerate((o0_ref, o1_ref, o2_ref, o3_ref)):
        n_tok = ref.shape[1]
        ref[0] = x_two[k * n_tok:(k + 1) * n_tok]
    d_h = dacc_ref[...].astype(HALF).astype(WIDE)
    d_ln, d_scale, d_bias = normalize_back(x_ref[...].astype(WIDE), scale_ref[1:2, :].astype(WIDE), d_h)
    d_x = (pack_ref[:, 2 * dim:].astype(WIDE) + d_ln).astype(HALF)
    dx_ref[...] = d_x
    sum_ref[...] += jnp.concatenate([d_scale, d_bias, jnp.sum(d_x.astype(WIDE), axis=0, keepdims=True), jnp.zeros((5, dim), WIDE)], axis=0)


def mlp(h_val, d_blocks, x_val, b2, scale, biases, near_ws, x_ws, diag_ws):
    (rows, dim), cols, tile = h_val.shape, near_ws[0].shape[2], 256
    far = [*near_ws, *x_ws, *diag_ws]
    specs = [tiled(tile, dim)] * 2 + [held(b2.shape), held(scale.shape)] + image_blocks(d_blocks) + extra_blocks(biases) + [pl.BlockSpec(memory_space=pl.ANY)] * len(far)
    outs = [shape_of(*val.shape) for val in d_blocks] + [shape_of(rows, width) for width in (2 * cols, 3 * dim, dim)] + [shape_of(8, width, dtype=WIDE) for width in (dim, cols)]
    scratch = [pltpu.VMEM((tile, cols), HALF)] * 2 + [pltpu.VMEM((tile, dim), WIDE)] * 2 + [pltpu.VMEM((4, 4) + x_ws[0].shape, HALF), pltpu.SemaphoreType.DMA((4, 4))]
    return run(mlp_kernel, rows // tile, specs, image_blocks(d_blocks) + [tiled(tile, o.shape[1]) for o in outs[4:7]] + [fixed(o.shape) for o in outs[7:]], outs,
               32 * rows * dim * cols, scratch)(h_val, x_val, b2, scale, *d_blocks, *biases, *far)


def grad_kernel(la_ref, lb_ref, ra_ref, rb_ref, *out_refs):
    first_step(*out_refs)
    width = out_refs[0].shape[1]
    for rows in chunks(out_refs[0].shape[0]):
        for at, out_ref in enumerate(out_refs):
            cols = slice(width * at, width * (at + 1))
            out_ref[rows, :] += mm_tn(la_ref[:, rows], ra_ref[:, cols]) + mm_tn(lb_ref[:, rows], rb_ref[:, cols])


def grad(ops, count):
    (lhs, dim, _), _, (_, size, _), _ = ops
    rows, tile, width = lhs.shape[0], 512, size // count
    out = shape_of(dim, width, dtype=WIDE)
    return run(grad_kernel, rows // tile, [block(tile, size, at) for _, size, at in ops], [fixed(out.shape)] * count, [out] * count,
               4 * count * rows * dim * width)(*[val for val, _, _ in ops])


def grad_mlp_kernel(ha_ref, ga_ref, da_ref, hb_ref, gb_ref, db_ref, hx_ref, dx_ref, hd_ref, dd_ref, w1_ref, b1_ref, w2_ref,
                    out1_ref, out2_ref, bsum_ref, acc1_ref, acc2_ref, g_ref, p_ref):
    first_step(bsum_ref, acc1_ref, acc2_ref)
    cols_n = w1_ref.shape[1]
    for at, (h_ref, d_ref) in enumerate(((hx_ref, dx_ref), (hd_ref, dd_ref))):
        def store(cols, hidden, d_pre):
            g_ref[at, :, cols] = hidden
            p_ref[at, :, cols] = d_pre.astype(HALF)
            bsum_ref[:, cols] += jnp.sum(d_pre, axis=0, keepdims=True)

        up(h_ref[...], d_ref[...], lambda cols: w1_ref[:, cols], b1_ref[...].astype(WIDE), lambda cols: w2_ref[cols, :], store)
    for rows in chunks(acc1_ref.shape[0]):
        acc1_ref[rows, :] += mm_tn(ha_ref[:, rows], ga_ref[:, cols_n:]) + mm_tn(hb_ref[:, rows], gb_ref[:, cols_n:]) + mm_tn(hx_ref[:, rows], p_ref[0]) + mm_tn(hd_ref[:, rows], p_ref[1])
    for rows in chunks(acc2_ref.shape[0]):
        acc2_ref[rows, :] += mm_tn(ga_ref[:, rows], da_ref[...]) + mm_tn(gb_ref[:, rows], db_ref[...]) + mm_tn(g_ref[0, :, rows], dx_ref[...]) + mm_tn(g_ref[1, :, rows], dd_ref[...])

    @pl.when(pl.program_id(0) == pl.num_programs(0) - 1)
    def _():
        out1_ref[...] = acc1_ref[...].astype(HALF)
        out2_ref[...] = acc2_ref[...].astype(HALF)


def grad_mlp(ops, w1, b1, w2):
    rows, (dim, cols), tile = ops[0][0].shape[0], w1.shape, 256
    outs = [shape_of(dim, cols), shape_of(cols, dim), shape_of(1, cols, dtype=WIDE)]
    scratch = [pltpu.VMEM((dim, cols), WIDE), pltpu.VMEM((cols, dim), WIDE)] + [pltpu.VMEM((2, tile, cols), HALF)] * 2
    return run(grad_mlp_kernel, rows // tile, [block(tile, width, at) for _, width, at in ops] + [held(w1.shape), held(b1.shape), held(w2.shape)],
               [fixed(o.shape) for o in outs], outs, 24 * rows * dim * cols, scratch)(*[val for val, _, _ in ops], w1, b1, w2)


def gather_pieces(piece):
    group = lax.axis_index('dp')
    pieces = [(x_swap(piece), group)]
    for hop, at in enumerate((group + 1 - 2 * (group % 2), (group + 2) % 4, 3 - group), 1):
        pieces.append((lax.ppermute(pieces[0][0], 'dp', [(i, i ^ hop) for i in range(4)]), at))
    return pieces


def after(vals, done):
    return lax.optimization_barrier((vals, done))[0]


def group_step(patches, patch_w, patch_b, pos_emb, ln_scale, ln_bias, qkv_w, qkv_b, out_w, out_b, fc1_w, fc1_b, fc2_w, fc2_b, d_out):
    n_img, n_tok, patch_dim = patches.shape
    dim = patch_w.shape[1]
    n_own = n_img // 4
    rows = n_own * 4 * n_tok
    cols = fc1_w.shape[1]
    group, me = lax.axis_index('dp'), lax.axis_index('tp')
    core = me % 2
    core_set = me + 1 - 2 * core
    sets = (me, core_set, (me + 2) % 4, (core_set + 2) % 4)

    def images(val, which):
        return lax.dynamic_slice_in_dim(val, sets[which] * n_own, n_own, 0)

    def quarter(val):
        part = val.shape[0] // 4
        return lax.dynamic_slice_in_dim(val, group * part, part, 0)

    row = lambda val: val.reshape(1, val.shape[-1])

    heads = qkv_w.shape[2] * qkv_w.shape[3]
    attn_w = jnp.concatenate([jnp.swapaxes(qkv_w, 0, 1).reshape(dim, 3 * heads), out_w.reshape(heads, dim).T], axis=1)
    attn_pieces = gather_pieces(quarter(attn_w))
    flat = jnp.concatenate([qkv_b.reshape(3 * heads), jnp.zeros((1024 - 3 * heads,), HALF), fc1_b]).reshape(4, 512)
    beside = jnp.concatenate([pos_emb[:, patch_dim:], jnp.pad(flat, ((0, n_tok - 4), (0, 0)))], axis=1)
    extra = jnp.stack([pos_emb[:, :patch_dim], beside])
    with_extra = lambda which: jnp.concatenate([images(patches, which), extra], axis=0)
    got = (with_extra(0), core_swap(with_extra(1)), x_swap(with_extra(2)), diag_swap(with_extra(3)))
    mlp_pieces = gather_pieces(jnp.stack([quarter(fc1_w), quarter(fc2_w)]))
    d_blocks = (images(d_out, 0), core_swap(images(d_out, 1)), x_swap(images(d_out, 2)), diag_swap(images(d_out, 3)))
    attn_c = core_swap(attn_w)
    fc1_c, fc2_c = core_swap(fc1_w), core_swap(fc2_w)

    attn_x = jnp.zeros_like(attn_w)
    for val, at in attn_pieces:
        attn_x = lax.dynamic_update_slice(attn_x, val, (at * (dim // 4), 0))
    attn_d = core_swap(attn_x)
    mlp_x = [val for val, _ in mlp_pieces]
    mlp_d = [core_swap(val) for val in mlp_x]
    mlp_near = [val.reshape(4, dim // 4, cols) for val in (fc1_w, fc2_w, fc1_c, fc2_c)]
    attn_ws = (attn_w, attn_x, attn_c, attn_d)

    emb, qkv, ctx, x_one, h_two, pack_f = front(got, patch_w, row(patch_b), ln_scale, ln_bias, row(out_b), attn_ws)
    h_two_x = x_swap(h_two)
    pack_f_c = core_swap(pack_f)
    h_two_d = core_swap(h_two_x)

    *x_blocks, own_gp, pack_m, d_x, sums_two, b_sums = mlp(h_two, d_blocks, x_one, row(fc2_b), ln_scale, (got[0], got[2], got[1], got[3]), mlp_near, mlp_x, mlp_d)
    pack_m_c = core_swap(pack_m)
    x_parts = (x_blocks[0], core_swap(x_blocks[1]), x_swap(x_blocks[2]), diag_swap(x_blocks[3]))
    d_x_c = core_swap(d_x)
    d_o_own, d_o_x = grad(((d_x, dim, 0), (d_x_c, dim, 0), (ctx, 2 * heads, 0), (pack_f_c, 2 * heads, 4)), 2)
    d_o_recv = x_swap(d_o_x)
    d_near, d_far, d_patch_part, d_pos_all, sums_one, d_qkv_sum = rear(qkv, d_x, emb, got, ln_scale, attn_ws)
    d_far_c = core_swap(d_far)
    third = 3 * heads
    d_qkv_x, = grad(((pack_f, dim, 0), (pack_f_c, dim, 0), (d_near, third, 1), (d_far_c, third, 1)), 1)
    d_qkv_recv = x_swap(d_qkv_x)
    d_qkv_own, = grad(((pack_f, dim, 0), (pack_f_c, dim, 0), (d_near, third, 0), (d_far_c, third, 0)), 1)

    def in_order(flip, low, high):
        return jnp.where(flip == 0, jnp.concatenate([low, high], axis=0), jnp.concatenate([high, low], axis=0))

    x_parts = after(x_parts, d_qkv_x)
    x_two_out = in_order(me // 2, in_order(core, x_parts[0], x_parts[1]), in_order(core, x_parts[2], x_parts[3]))

    d_parts = (x_swap(images(d_out, 0)), diag_swap(images(d_out, 1)), images(d_out, 2), core_swap(images(d_out, 3)))
    d_oth = jnp.concatenate(after(d_parts, d_qkv_x), axis=1).reshape(rows, dim)
    d_oth_d = core_swap(d_oth)
    d_fc1_w, d_fc2_w, sum_other = grad_mlp((
        (h_two, dim, 0), (own_gp, 2 * cols, 0), (pack_m, dim, 2), (pack_f_c, dim, 1), (pack_m_c, 2 * cols, 0), (pack_m_c, dim, 2),
        (h_two_x, dim, 0), (d_oth, dim, 0), (h_two_d, dim, 0), (d_oth_d, dim, 0)), fc1_w, row(fc1_b), fc2_w)
    d_fc2_b = jnp.sum(d_out, axis=(0, 1), dtype=WIDE)

    half_rows = patch_dim // 2
    mine = lax.dynamic_slice_in_dim(d_patch_part, core * half_rows, half_rows, 0)
    theirs = lax.dynamic_slice_in_dim(d_patch_part, (1 - core) * half_rows, half_rows, 0)
    mine = mine + core_swap(theirs)
    mine = (mine + x_swap(mine)).astype(HALF)
    theirs = core_swap(mine)
    d_patch_w = jnp.where(core == 0, jnp.concatenate([mine, theirs]), jnp.concatenate([theirs, mine]))

    d_pos_all, d_qkv_sum, sums_one = after((d_pos_all, d_qkv_sum, sums_one), d_qkv_x)
    d_patch_b = jnp.sum(d_pos_all, axis=0, keepdims=True)
    small = jnp.concatenate([sums_one[:1], sums_two[:1], sums_one[1:2], sums_two[1:2], sums_two[2:3], d_patch_b, row(d_fc2_b)], axis=0)
    wide_row = lambda side: jnp.pad(d_qkv_sum[:, 3 * heads * side:3 * heads * (side + 1)], ((0, 0), (0, dim - 3 * heads)))
    pos_block = lambda at: d_pos_all[at * n_tok:(at + 1) * n_tok]
    from_core = core_swap(jnp.concatenate([pos_block(1), pos_block(3), small, wide_row(2), wide_row(3), b_sums[1:2]], axis=0))
    mine_sum = jnp.concatenate([pos_block(0), pos_block(2), small, wide_row(0), wide_row(1), b_sums[:1]], axis=0) + from_core
    d_fc1_b = mine_sum[2 * n_tok + 9] + sum_other[0]
    small = mine_sum[2 * n_tok:2 * n_tok + 7]
    from_x = x_swap(jnp.concatenate([mine_sum[n_tok:2 * n_tok], small, mine_sum[2 * n_tok + 8:2 * n_tok + 9]], axis=0))
    total = (jnp.concatenate([mine_sum[:n_tok], small, mine_sum[2 * n_tok + 7:2 * n_tok + 8]], axis=0) + from_x).astype(HALF)
    d_pos, small, d_qkv_b = total[:n_tok], total[n_tok:n_tok + 7], total[n_tok + 7, :3 * heads]

    d_qkv_w = jnp.swapaxes((d_qkv_own + d_qkv_recv).astype(HALF).reshape((dim,) + qkv_b.shape), 0, 1)
    d_out_w = (d_o_own + d_o_recv).astype(HALF).T.reshape(out_w.shape)
    return (x_two_out, d_patch_w, small[5], d_pos, small[:2], small[2:4], d_qkv_w, d_qkv_b.reshape(qkv_b.shape), d_out_w, small[4], d_fc1_w, d_fc1_b.astype(HALF), d_fc2_w, small[6])


def solution(mesh):
    in_specs = (P('dp', 'tp'), P(), P(), P('tp'), P(), P(), P(None, None, 'tp'), P(None, 'tp'), P('tp'), P(), P(None, 'tp'), P('tp'), P('tp'), P(), P('dp', 'tp'))
    out_specs = (P('dp', 'tp'), P('dp'), P('dp'), P(('dp', 'tp')), P('dp'), P('dp'), P('dp', None, 'tp'), P('dp', 'tp'), P(('dp', 'tp')), P('dp'), P('dp', 'tp'), P(('dp', 'tp')), P(('dp', 'tp')), P('dp'))
    return jax.shard_map(group_step, mesh=mesh, in_specs=in_specs, out_specs=out_specs, check_vma=False)
```
